32 devices in a mesh: dp: 16 (over z, x, core), blk: 2 (over y).
Axes of the slice: x: 2, y: 2, z: 4, core: 2. Of those that a mesh axis runs over, the one named last changes fastest.
Arguments:
- patches: bfloat16 [16, 1024, 768], P('dp', 'blk'), may hold values from -6 to 6
- vis_slot: int32 [16, 1024], P('dp', 'blk'), may hold values from 0 to 671, as said below
- seg_ids: int32 [16, 1344], P('dp', 'blk'), may hold values from 0 to 5, never falling along the last dimension, each value on 1 to 840 neighbouring positions
- enc_norm1_gain: bfloat16 [768], replicated, may hold values from 0.25 to 1.75
- enc_norm1_bias: bfloat16 [768], replicated, may hold values from -1.75 to 1.75
- enc_qkv_weight: bfloat16 [768, 2304], replicated, may hold values from -0.21875 to 0.21875
- enc_query_bias: bfloat16 [768], replicated, may hold values from -3 to 3
- enc_value_bias: bfloat16 [768], replicated, may hold values from -3 to 3
- enc_out_weight: bfloat16 [768, 768], replicated, may hold values from -0.875 to 0.875
- enc_out_bias: bfloat16 [768], replicated, may hold values from -1.75 to 1.75
- enc_norm2_gain: bfloat16 [768], replicated, may hold values from 0.25 to 1.75
- enc_norm2_bias: bfloat16 [768], replicated, may hold values from -1.75 to 1.75
- enc_up_weight: bfloat16 [768, 3072], replicated, may hold values from -0.21875 to 0.21875
- enc_up_bias: bfloat16 [3072], replicated, may hold values from -3 to 3
- enc_down_weight: bfloat16 [3072, 768], replicated, may hold values from -0.109375 to 0.109375
- enc_down_bias: bfloat16 [768], replicated, may hold values from -1.75 to 1.75
- emb_weight: bfloat16 [768, 512], replicated, may hold values from -0.21875 to 0.21875
- emb_bias: bfloat16 [512], replicated, may hold values from -3 to 3
- mask_token: bfloat16 [512], replicated, may hold values from -6 to 6
- dec_norm1_gain: bfloat16 [512], replicated, may hold values from 0.25 to 1.75
- dec_norm1_bias: bfloat16 [512], replicated, may hold values from -1.75 to 1.75
- dec_qkv_weight: bfloat16 [512, 1536], replicated, may hold values from -0.25 to 0.25
- dec_query_bias: bfloat16 [512], replicated, may hold values from -3 to 3
- dec_value_bias: bfloat16 [512], replicated, may hold values from -3 to 3
- dec_out_weight: bfloat16 [512, 512], replicated, may hold values from -1 to 1
- dec_out_bias: bfloat16 [512], replicated, may hold values from -3.5 to 3.5
- dec_norm2_gain: bfloat16 [512], replicated, may hold values from 0.25 to 1.75
- dec_norm2_bias: bfloat16 [512], replicated, may hold values from -1.75 to 1.75
- dec_up_weight: bfloat16 [512, 2048], replicated, may hold values from -0.25 to 0.25
- dec_up_bias: bfloat16 [2048], replicated, may hold values from -3 to 3
- dec_down_weight: bfloat16 [2048, 512], replicated, may hold values from -0.125 to 0.125
- dec_down_bias: bfloat16 [512], replicated, may hold values from -6 to 6
- cotangent: bfloat16 [16, 1344, 512], P('dp', 'blk'), may hold values from -6 to 6
Outputs:
- dec_out: bfloat16 [16, 1344, 512], P('dp', 'blk')
- grad_patches: bfloat16 [16, 1024, 768], P('dp', 'blk')
- grad_enc_norm1_gain: float32 [768], P('dp')
- grad_enc_norm1_bias: float32 [768], P('dp')
- grad_enc_qkv_weight: float32 [768, 2304], P('dp')
- grad_enc_query_bias: float32 [768], P('dp')
- grad_enc_value_bias: float32 [768], P('dp')
- grad_enc_out_weight: float32 [768, 768], P('dp')
- grad_enc_out_bias: float32 [768], P('dp')
- grad_enc_norm2_gain: float32 [768], P('dp')
- grad_enc_norm2_bias: float32 [768], P('dp')
- grad_enc_up_weight: float32 [768, 3072], P('dp')
- grad_enc_up_bias: float32 [3072], P('dp')
- grad_enc_down_weight: float32 [3072, 768], P('dp')
- grad_enc_down_bias: float32 [768], P('dp')
- grad_emb_weight: float32 [768, 512], P('dp')
- grad_emb_bias: float32 [512], P('dp')
- grad_mask_token: float32 [512], P('dp')
- grad_dec_norm1_gain: float32 [512], P('dp')
- grad_dec_norm1_bias: float32 [512], P('dp')
- grad_dec_qkv_weight: float32 [512, 1536], P('dp')
- grad_dec_query_bias: float32 [512], P('dp')
- grad_dec_value_bias: float32 [512], P('dp')
- grad_dec_out_weight: float32 [512, 512], P('dp')
- grad_dec_out_bias: float32 [512], P('dp')
- grad_dec_norm2_gain: float32 [512], P('dp')
- grad_dec_norm2_bias: float32 [512], P('dp')
- grad_dec_up_weight: float32 [512, 2048], P('dp')
- grad_dec_up_bias: float32 [2048], P('dp')
- grad_dec_down_weight: float32 [2048, 512], P('dp')
- grad_dec_down_bias: float32 [512], P('dp')
The draws below stay inside these ranges and needn't reach their ends.
Inputs may be any that keep to these rules, and one draw needn't show every extreme that they name: `vis_slot`: in every strip, each aligned run of 512 entries lists distinct positions in increasing order within one block of 672 positions; the block's first and last positions are always listed. `seg_ids`: segment ids never fall along a strip; a segment spans 1 to 840 positions.
All inputs are finite; a program needn't handle non-finite values.
Results may differ from the reference program's by a relative error of at most 0.025.
Values may be sent and summed in bfloat16 or wider, within the bound.
A program may use at most 384 MiB of HBM per device.

```python
import math
import jax
import jax.numpy as jnp
import numpy as np
from jax import lax

D_ENC = 768
HEADS_ENC = 12
FF_ENC = 3072
D_DEC = 512
HEADS_DEC = 16
FF_DEC = 2048
VIS = 1024
PATCHES = 1344
STRIPS = 16
VIS_DEV = 512
P_DEV = 672


def draw_vis_slot(key, part):
    runs = VIS // VIS_DEV
    blocks = STRIPS * runs
    inner = P_DEV - 2
    scores = jax.random.randint(key, (blocks, inner), 0, 2097152)
    scores = scores * inner + jnp.arange(inner, dtype=jnp.int32)[None, :]
    picked = jnp.argsort(scores, axis=1)[:, :VIS_DEV - 2].astype(jnp.int32) + 1
    first_col = jnp.zeros((blocks, 1), jnp.int32)
    last_col = jnp.full((blocks, 1), P_DEV - 1, jnp.int32)
    joined = jnp.concatenate([first_col, picked, last_col], axis=1)
    return jnp.sort(joined, axis=1).reshape(STRIPS, VIS).astype(jnp.int32)


def levels(key, dims, pieces, smallest, largest):
    level, own = 1.0, jax.random.fold_in(key, 6)
    for dim, shards_of in pieces:
        steps = jnp.exp(jax.random.uniform(jax.random.fold_in(own, dim), (shards_of,), jnp.float32, smallest / len(pieces), largest / len(pieces)))
        level = level * jnp.repeat(steps, dims[dim] // shards_of).reshape([-1 if axis == dim else 1 for axis in range(len(dims))])
    return level


def length_profile(amount, total, limit, slope):
    portions = [(1 << 20) // math.isqrt(rank ** slope) + 1 for rank in range(2, amount + 1)]
    spare, holding = total - limit - (amount - 1), [1] * (amount - 1)
    while spare > 0:
        candidates = [i for i in range(amount - 1) if holding[i] < limit]
        mass, budget = sum([portions[i] for i in candidates]), spare
        for i in candidates:
            more = min(limit - holding[i], max(1, budget * portions[i] // mass), spare)
            holding[i] = holding[i] + more
            spare = spare - more
    return np.array([limit] + holding)


def ragged(rng, amount, total, bound, lean):
    if amount == 2:
        one = jax.random.randint(rng, (), max(1, total - bound), min(bound, total - 1) + 1)
        return jnp.stack([one, total - one])
    sizes = jnp.asarray(length_profile(amount, total, bound, lean), jnp.int32)
    couples = (amount - 1) // 2
    source_of, receiver = sizes[1:1 + 2 * couples:2], sizes[2:2 + 2 * couples:2]
    margin = jnp.minimum(source_of - 1, bound - receiver)
    passed = jax.random.randint(jax.random.fold_in(rng, 1), (couples,), 0, 1 << 20) % (margin + 1)
    sizes = sizes.at[1:1 + 2 * couples:2].set(source_of - passed).at[2:2 + 2 * couples:2].set(receiver + passed)
    return sizes[jax.random.permutation(jax.random.fold_in(rng, 2), amount)]


def scatter_about(key, dims, scale, reach, split=(), held_as=jnp.bfloat16):
    level = levels(key, dims, split, -0.22, 0.18) if split else 1.0
    result = jax.random.normal(key, dims, jnp.float32) * scale * level
    return jnp.minimum(jnp.maximum(result, -reach), reach).astype(held_as)


def setup_inputs(seed: int = 0) -> dict:
    splits = jax.random.split(jax.random.key(seed), 34)
    return {
        "patches": scatter_about(splits[0], (STRIPS, VIS, D_ENC), 1.0, 6.0, ((0, 16), (1, 2))),
        "vis_slot": draw_vis_slot(jax.random.fold_in(splits[33], 71), 0),
        "seg_ids": jax.vmap(lambda own: jnp.searchsorted(jnp.cumsum(ragged(own, 6, PATCHES, PATCHES * 5 // 8, 0)), jnp.arange(PATCHES), side="right"))(jax.random.split(splits[2], STRIPS)).reshape((STRIPS, PATCHES)).astype(jnp.int32),
        "enc_norm1_gain": jnp.clip(1.0 + 0.15 * jax.random.normal(splits[3], (D_ENC,), jnp.float32), 0.25, 1.75).astype(jnp.bfloat16),
        "enc_norm1_bias": scatter_about(splits[4], (D_ENC,), 0.3, 1.75),
        "enc_qkv_weight": scatter_about(splits[5], (D_ENC, 3 * D_ENC), D_ENC ** -0.5, 0.21875),
        "enc_query_bias": scatter_about(splits[6], (D_ENC,), 0.5, 3.0),
        "enc_value_bias": scatter_about(splits[7], (D_ENC,), 0.5, 3.0),
        "enc_out_weight": scatter_about(splits[8], (D_ENC, D_ENC), (D_ENC // 16) ** -0.5, 0.875),
        "enc_out_bias": scatter_about(splits[9], (D_ENC,), 0.3, 1.75),
        "enc_norm2_gain": jnp.clip(1.0 + 0.15 * jax.random.normal(splits[10], (D_ENC,), jnp.float32), 0.25, 1.75).astype(jnp.bfloat16),
        "enc_norm2_bias": scatter_about(splits[11], (D_ENC,), 0.3, 1.75),
        "enc_up_weight": scatter_about(splits[12], (D_ENC, FF_ENC), D_ENC ** -0.5, 0.21875),
        "enc_up_bias": scatter_about(splits[13], (FF_ENC,), 0.5, 3.0),
        "enc_down_weight": scatter_about(splits[14], (FF_ENC, D_ENC), FF_ENC ** -0.5, 0.109375),
        "enc_down_bias": scatter_about(splits[15], (D_ENC,), 0.3, 1.75),
        "emb_weight": scatter_about(splits[16], (D_ENC, D_DEC), D_ENC ** -0.5, 0.21875),
        "emb_bias": scatter_about(splits[17], (D_DEC,), 0.5, 3.0),
        "mask_token": scatter_about(splits[18], (D_DEC,), 1.0, 6.0),
        "dec_norm1_gain": jnp.clip(1.0 + 0.15 * jax.random.normal(splits[19], (D_DEC,), jnp.float32), 0.25, 1.75).astype(jnp.bfloat16),
        "dec_norm1_bias": scatter_about(splits[20], (D_DEC,), 0.3, 1.75),
        "dec_qkv_weight": scatter_about(splits[21], (D_DEC, 3 * D_DEC), D_DEC ** -0.5, 0.25),
        "dec_query_bias": scatter_about(splits[22], (D_DEC,), 0.5, 3.0),
        "dec_value_bias": scatter_about(splits[23], (D_DEC,), 0.5, 3.0),
        "dec_out_weight": scatter_about(splits[24], (D_DEC, D_DEC), (D_DEC // 16) ** -0.5, 1.0),
        "dec_out_bias": scatter_about(splits[25], (D_DEC,), 0.6, 3.5),
        "dec_norm2_gain": jnp.clip(1.0 + 0.15 * jax.random.normal(splits[26], (D_DEC,), jnp.float32), 0.25, 1.75).astype(jnp.bfloat16),
        "dec_norm2_bias": scatter_about(splits[27], (D_DEC,), 0.3, 1.75),
        "dec_up_weight": scatter_about(splits[28], (D_DEC, FF_DEC), D_DEC ** -0.5, 0.25),
        "dec_up_bias": scatter_about(splits[29], (FF_DEC,), 0.5, 3.0),
        "dec_down_weight": scatter_about(splits[30], (FF_DEC, D_DEC), FF_DEC ** -0.5, 0.125),
        "dec_down_bias": scatter_about(splits[31], (D_DEC,), 1.0, 6.0),
        "cotangent": scatter_about(splits[32], (STRIPS, PATCHES, D_DEC), 1.0, 6.0, ((0, 16), (1, 2))),
    }


@jax.custom_vjp
def low(v):
    return lax.optimization_barrier(v.astype(jnp.bfloat16)).astype(jnp.float32)

@jax.custom_vjp
def low_back(v):
    return v

def low_keep(v):
    return (low(v), None)

def low_pass(kept, grad):
    return (grad,)

def back_keep(v):
    return (v, None)

def back_low(kept, grad):
    return (low(grad),)
low.defvjp(low_keep, low_pass)
low_back.defvjp(back_keep, back_low)
EPSILON = 1e-06

def product(left, right):
    return jnp.dot(left, right, precision=lax.Precision.HIGHEST)

def layer_norm(values, gain, bias):
    centre = lax.optimization_barrier(jnp.mean(values, axis=-1, keepdims=True))
    centred = values - centre
    spread = lax.optimization_barrier(jnp.mean(centred * centred, axis=-1, keepdims=True))
    return centred * lax.rsqrt(spread + EPSILON) * gain + bias

def attention(queries, key_rows, value_rows, segments, head_count):
    rows_here, model_width = queries.shape
    head_size = model_width // head_count
    query_heads = queries.reshape(rows_here, head_count, head_size)
    key_heads = key_rows.reshape(rows_here, head_count, head_size)
    value_heads = value_rows.reshape(rows_here, head_count, head_size)
    scores = jnp.einsum('rhd,khd->hrk', query_heads, key_heads, precision=lax.Precision.HIGHEST) * head_size ** (-0.5)
    scores = low_back(scores)
    allowed = segments[:, None] == segments[None, :]
    scores = jnp.where(allowed[None], scores, -1e+30)
    peak = lax.optimization_barrier(jnp.max(scores, axis=-1, keepdims=True))
    raised = jnp.exp(scores - peak)
    probs = low(raised / lax.optimization_barrier(jnp.sum(raised, axis=-1, keepdims=True)))
    mixed = jnp.einsum('hrk,khd->rhd', probs, value_heads, precision=lax.Precision.HIGHEST)
    return mixed.reshape(rows_here, model_width)

def block(residual, segments, weights, head_count):
    norm1_gain, norm1_bias, qkv_weight, query_bias, value_bias, out_weight, out_bias, norm2_gain, norm2_bias, up_weight, up_bias, down_weight, down_bias = weights
    model_width = residual.shape[-1]
    normed = low(layer_norm(residual, norm1_gain, norm1_bias))
    projected = product(normed, qkv_weight)
    queries = low(low_back(projected[:, :model_width] + query_bias))
    key_rows = low(low_back(projected[:, model_width:2 * model_width]))
    value_rows = low(low_back(projected[:, 2 * model_width:] + value_bias))
    attended = low(low_back(attention(queries, key_rows, value_rows, segments, head_count)))
    middle = residual + low_back(product(attended, out_weight) + out_bias)
    normed_two = low(layer_norm(middle, norm2_gain, norm2_bias))
    pre_act = low_back(product(normed_two, up_weight) + up_bias)
    hidden = low(jax.nn.gelu(pre_act, approximate=False))
    return middle + low_back(product(hidden, down_weight) + down_bias)

def strip_layers(patch_rows, slots, segments, params):
    enc_weights = params[0:13]
    emb_weight, emb_bias, mask_token = (params[13], params[14], params[15])
    dec_weights = params[16:29]
    positions = jnp.arange(VIS, dtype=jnp.int32) // VIS_DEV * P_DEV + slots.astype(jnp.int32)
    vis_segments = segments[positions]
    encoded = low(block(patch_rows, vis_segments, enc_weights, HEADS_ENC))
    shown = low_back(product(encoded, emb_weight)) + emb_bias
    start_rows = jnp.broadcast_to(mask_token, (PATCHES, D_DEC))
    dec_in = start_rows.at[positions].set(shown)
    return block(dec_in, segments, dec_weights, HEADS_DEC)

def reference(patches, vis_slot, seg_ids, enc_norm1_gain, enc_norm1_bias, enc_qkv_weight, enc_query_bias, enc_value_bias, enc_out_weight, enc_out_bias, enc_norm2_gain, enc_norm2_bias, enc_up_weight, enc_up_bias, enc_down_weight, enc_down_bias, emb_weight, emb_bias, mask_token, dec_norm1_gain, dec_norm1_bias, dec_qkv_weight, dec_query_bias, dec_value_bias, dec_out_weight, dec_out_bias, dec_norm2_gain, dec_norm2_bias, dec_up_weight, dec_up_bias, dec_down_weight, dec_down_bias, cotangent):
    raw_params = (enc_norm1_gain, enc_norm1_bias, enc_qkv_weight, enc_query_bias, enc_value_bias, enc_out_weight, enc_out_bias, enc_norm2_gain, enc_norm2_bias, enc_up_weight, enc_up_bias, enc_down_weight, enc_down_bias, emb_weight, emb_bias, mask_token, dec_norm1_gain, dec_norm1_bias, dec_qkv_weight, dec_query_bias, dec_value_bias, dec_out_weight, dec_out_bias, dec_norm2_gain, dec_norm2_bias, dec_up_weight, dec_up_bias, dec_down_weight, dec_down_bias)
    params = tuple((param.astype(jnp.float32) for param in raw_params))

    def forward(inputs, weights):

        def one_strip(item):
            return jax.checkpoint(strip_layers)(item[0], item[1], item[2], weights)
        return lax.map(one_strip, (inputs, vis_slot, seg_ids))
    outputs, pull = jax.vjp(forward, patches.astype(jnp.float32), params)
    grad_inputs, grads = pull(cotangent.astype(jnp.float32))
    return (outputs.astype(jnp.bfloat16), grad_inputs.astype(jnp.bfloat16), grads[0], grads[1], grads[2], grads[3], grads[4], grads[5], grads[6], grads[7], grads[8], grads[9], grads[10], grads[11], grads[12], grads[13], grads[14], grads[15], grads[16], grads[17], grads[18], grads[19], grads[20], grads[21], grads[22], grads[23], grads[24], grads[25], grads[26], grads[27], grads[28])
```

```python
import functools
import jax
import jax.numpy as jnp
from jax import lax
from jax.experimental import pallas as pl
from jax.experimental.pallas import tpu as pltpu
from jax.sharding import PartitionSpec as P

HEADS_ENC = 12
HEADS_DEC = 16

LN2 = 0.6931471805599453
BIG = -(2.0 ** 100)
NT = (((1,), (1,)), ((), ()))
BQ = 256
BK = 256


def padded_rows(rows):
    return -(-rows // 128) * 128 + 128


def key_ranges(segments, rows):
    blocks = -(-rows // BQ)
    filled = jnp.concatenate([segments, jnp.full((blocks * BQ - rows,), 7, jnp.int32)])
    filled = jnp.minimum(filled, segments[rows - 1]).reshape(blocks, BQ)
    low = jnp.sum(segments[None, :] < filled[:, 0:1], axis=1)
    high = jnp.sum(segments[None, :] <= filled[:, BQ - 1 :], axis=1)
    start = low // 128
    count = (high - start * 128 + BK - 1) // BK
    return jnp.concatenate([start, count]).astype(jnp.int32)


def lanes(rows, width=128):
    return lax.broadcasted_iota(jnp.int32, (rows, width), 1)


def attention_forward_kernel(
    rows, head_size, ranges, q_ref, k_ref, v_ref, seg_ref, out_ref, lse_ref, ka, va, qa, sc, acc
):
    heads = 128 // head_size
    group = pl.program_id(0)
    block = pl.program_id(1)
    blocks = pl.num_programs(1)
    padded = ka.shape[0]

    @pl.when(block == 0)
    def _():
        marks = jnp.where(lanes(rows) == seg_ref[0:rows, :], 0.0, BIG)
        marks = jnp.where(lanes(rows) < 8, marks, 0.0)
        ka[0:rows, 0:128] = k_ref[...]
        ka[0:rows, 128:256] = marks.astype(jnp.bfloat16)
        va[0:rows, 0:128] = v_ref[...]
        va[0:rows, 128:256] = jnp.ones((rows, 128), jnp.bfloat16)
        rest = padded - rows
        ka[rows:padded, 0:128] = jnp.zeros((rest, 128), jnp.bfloat16)
        ka[rows:padded, 128:256] = jnp.where(lanes(rest) < 8, BIG, 0.0).astype(jnp.bfloat16)
        va[rows:padded, :] = jnp.zeros((rest, 256), jnp.bfloat16)

    first = pl.multiple_of(block * BQ, BQ)
    lane = lanes(BQ)
    marks = jnp.where(lane == seg_ref[pl.ds(first, BQ), :], 1.0, 0.0).astype(jnp.bfloat16)
    queries = q_ref[...]
    for head in range(heads):
        here = lane // head_size == head
        qa[head * BQ : (head + 1) * BQ, 0:128] = jnp.where(here, queries, jnp.zeros_like(queries))
        qa[head * BQ : (head + 1) * BQ, 128:256] = marks

    start = ranges[block] * 128
    count = ranges[blocks + block]

    def score(step, peak):
        at = pl.multiple_of(start + step * BK, 128)
        s = lax.dot_general(qa[...], ka[pl.ds(at, BK), :], NT, preferred_element_type=jnp.float32)
        sc[step] = s
        return jnp.maximum(peak, jnp.maximum(s[:, 0:128], s[:, 128:256]))

    peak = lax.fori_loop(0, count, score, jnp.full((heads * BQ, 128), BIG, jnp.float32))
    top = jnp.max(peak, axis=1, keepdims=True)
    acc[...] = jnp.zeros_like(acc)

    def weigh(step, carry):
        at = pl.multiple_of(start + step * BK, 128)
        p = jnp.exp2(sc[step] - top).astype(jnp.bfloat16)
        acc[...] += jnp.dot(p, va[pl.ds(at, BK), :], preferred_element_type=jnp.float32)
        return carry

    lax.fori_loop(0, count, weigh, 0)
    out = jnp.zeros((BQ, 128), jnp.float32)
    lse = jnp.zeros((BQ, 128), jnp.float32)
    for head in range(heads):
        part = acc[head * BQ : (head + 1) * BQ, :]
        total = part[:, 128:256]
        out = jnp.where(lane // head_size == head, part[:, 0:128] / total, out)
        lse = jnp.where(lane == 16 + head, top[head * BQ : (head + 1) * BQ] + jnp.log2(total), lse)
    out_ref[...] = out.astype(jnp.bfloat16)
    lse_ref[...] = lse


def attention_forward(qkv, segments, ranges, head_size):
    rows, width = qkv.shape
    groups = width // 384
    blocks = -(-rows // BQ)
    padded = padded_rows(rows)
    heads = 128 // head_size
    steps = -(-padded // BK)
    seg_column = jnp.concatenate(
        [segments, jnp.full((blocks * BQ - rows,), 7, jnp.int32)]
    ).reshape(-1, 1)
    return pl.pallas_call(
        functools.partial(attention_forward_kernel, rows, head_size),
        grid_spec=pltpu.PrefetchScalarGridSpec(
            num_scalar_prefetch=1,
            grid=(groups, blocks),
            in_specs=[
                pl.BlockSpec((BQ, 128), lambda g, i, r: (i, g)),
                pl.BlockSpec((rows, 128), lambda g, i, r: (0, groups + g)),
                pl.BlockSpec((rows, 128), lambda g, i, r: (0, 2 * groups + g)),
                pl.BlockSpec((blocks * BQ, 1), lambda g, i, r: (0, 0)),
            ],
            out_specs=[
                pl.BlockSpec((BQ, 128), lambda g, i, r: (i, g)),
                pl.BlockSpec((BQ, 128), lambda g, i, r: (i, g)),
            ],
            scratch_shapes=[
                pltpu.VMEM((padded, 256), jnp.bfloat16),
                pltpu.VMEM((padded, 256), jnp.bfloat16),
                pltpu.VMEM((heads * BQ, 256), jnp.bfloat16),
                pltpu.VMEM((steps, heads * BQ, BK), jnp.float32),
                pltpu.VMEM((heads * BQ, 256), jnp.float32),
            ],
        ),
        out_shape=[
            jax.ShapeDtypeStruct((rows, groups * 128), jnp.bfloat16),
            jax.ShapeDtypeStruct((rows, groups * 128), jnp.float32),
        ],
        name="attention_forward",
    )(ranges, qkv, qkv, qkv, seg_column)


def spread(values):
    high = values.astype(jnp.bfloat16).astype(jnp.float32)
    middle = (values - high).astype(jnp.bfloat16).astype(jnp.float32)
    low = values - high - middle
    return high + pltpu.roll(middle, 16, 1) + pltpu.roll(low, 32, 1)


def attention_backward_kernel(
    rows, head_size, ranges, q_ref, k_ref, v_ref, o_ref, do_ref, lse_ref, seg_ref,
    dqkv_ref, bias_ref, ka, va, qa, da, qt, dt, dkt, dvt, dq
):
    heads = 128 // head_size
    group = pl.program_id(0)
    groups = pl.num_programs(0)
    block = pl.program_id(1)
    blocks = pl.num_programs(1)
    padded = ka.shape[0]
    scale = float(head_size) ** -0.5

    @pl.when(block == 0)
    def _():
        lane = lanes(rows)
        marks = jnp.where(lane == seg_ref[0:rows, :], 0.0, BIG)
        ones = jnp.where((lane >= 16) & (lane < 64), 1.0, 0.0)
        ka[0:rows, 0:128] = k_ref[...]
        ka[0:rows, 128:256] = jnp.where(lane < 8, marks, ones).astype(jnp.bfloat16)
        va[0:rows, 0:128] = v_ref[...]
        va[0:rows, 128:256] = ones.astype(jnp.bfloat16)
        rest = padded - rows
        ka[rows:padded, 0:128] = jnp.zeros((rest, 128), jnp.bfloat16)
        ka[rows:padded, 128:256] = jnp.where(lanes(rest) < 8, BIG, 0.0).astype(jnp.bfloat16)
        va[rows:padded, :] = jnp.zeros((rest, 256), jnp.bfloat16)
        dkt[...] = jnp.zeros_like(dkt)
        dvt[...] = jnp.zeros_like(dvt)

    first = pl.multiple_of(block * BQ, BQ)
    lane = lanes(BQ)
    left = rows - first
    inside = lax.broadcasted_iota(jnp.int32, (BQ, 128), 0) < left
    marks = jnp.where(lane == seg_ref[pl.ds(first, BQ), :], 1.0, 0.0)
    queries = jnp.where(inside, q_ref[...].astype(jnp.float32), 0.0)
    grads = jnp.where(inside, do_ref[...].astype(jnp.float32), 0.0)
    product = jnp.where(inside, grads * o_ref[...].astype(jnp.float32), 0.0)
    picks = (
        lax.broadcasted_iota(jnp.int32, (128, 128), 0) // head_size + 16
        == lax.broadcasted_iota(jnp.int32, (128, 128), 1)
    )
    picks = jnp.where(picks, 1.0, 0.0).astype(jnp.bfloat16)
    product_high = product.astype(jnp.bfloat16)
    product_low = (product - product_high.astype(jnp.float32)).astype(jnp.bfloat16)
    dots = jnp.dot(product_high, picks, preferred_element_type=jnp.float32) + jnp.dot(
        product_low, picks, preferred_element_type=jnp.float32
    )
    lse = jnp.where(inside, lse_ref[...], 0.0)
    lse_terms = spread(-lse)
    dot_terms = spread(-dots)
    qt[...] = queries.T.astype(jnp.bfloat16)
    dt[...] = grads.T.astype(jnp.bfloat16)
    for head in range(heads):
        here = lane // head_size == head
        own = (lane == 16 + head) | (lane == 32 + head) | (lane == 48 + head)
        at = slice(head * BQ, (head + 1) * BQ)
        qa[at, 0:128] = jnp.where(here, queries, 0.0).astype(jnp.bfloat16)
        qa[at, 128:256] = jnp.where(own, lse_terms, marks).astype(jnp.bfloat16)
        da[at, 0:128] = jnp.where(here, grads, 0.0).astype(jnp.bfloat16)
        da[at, 128:256] = jnp.where(own, dot_terms, 0.0).astype(jnp.bfloat16)
    dq[...] = jnp.zeros_like(dq)
    start = ranges[block] * 128
    count = ranges[blocks + block]

    def body(step, carry):
        at = pl.multiple_of(start + step * BK, 128)
        keys = ka[pl.ds(at, BK), :]
        values = va[pl.ds(at, BK), :]
        s = lax.dot_general(qa[...], keys, NT, preferred_element_type=jnp.float32)
        p = jnp.exp2(s)
        dp = lax.dot_general(da[...], values, NT, preferred_element_type=jnp.float32)
        ds = (p * dp).astype(jnp.bfloat16)
        p = p.astype(jnp.bfloat16)
        dq[...] += jnp.dot(ds, keys[:, 0:128], preferred_element_type=jnp.float32)
        for head in range(heads):
            rows_in = slice(head * BQ, (head + 1) * BQ)
            top = slice(head * head_size, (head + 1) * head_size)
            dvt[top, pl.ds(at, BK)] += jnp.dot(
                dt[top, :], p[rows_in], preferred_element_type=jnp.float32
            )
            dkt[top, pl.ds(at, BK)] += jnp.dot(
                qt[top, :], ds[rows_in], preferred_element_type=jnp.float32
            )
        return carry

    lax.fori_loop(0, count, body, 0)
    out = jnp.zeros((BQ, 128), jnp.float32)
    for head in range(heads):
        out = jnp.where(lane // head_size == head, dq[head * BQ : (head + 1) * BQ, :], out)
    out = jnp.where(inside, out * scale, 0.0)
    column = pl.multiple_of(group * 128, 128)

    @pl.when(block == 0)
    def _():
        bias_ref[:, pl.ds(column, 128)] = jnp.zeros((8, 128), jnp.float32)

    bias_ref[0:1, pl.ds(column, 128)] += jnp.sum(out, axis=0, keepdims=True)
    tail = rows - (rows // BQ) * BQ

    if tail == 0:
        dqkv_ref[pl.ds(first, BQ), pl.ds(column, 128)] = out.astype(jnp.bfloat16)
    else:
        @pl.when(block < blocks - 1)
        def _():
            dqkv_ref[pl.ds(first, BQ), pl.ds(column, 128)] = out.astype(jnp.bfloat16)

        @pl.when(block == blocks - 1)
        def _():
            dqkv_ref[rows - tail : rows, pl.ds(column, 128)] = out[0:tail].astype(jnp.bfloat16)

    @pl.when(block == blocks - 1)
    def _():
        k_column = pl.multiple_of((groups + group) * 128, 128)
        v_column = pl.multiple_of((2 * groups + group) * 128, 128)
        d_key = (dkt[...].T * LN2)[0:rows]
        d_value = dvt[...].T[0:rows]
        dqkv_ref[:, pl.ds(k_column, 128)] = d_key.astype(jnp.bfloat16)
        dqkv_ref[:, pl.ds(v_column, 128)] = d_value.astype(jnp.bfloat16)
        bias_ref[:, pl.ds(k_column, 128)] = jnp.zeros((8, 128), jnp.float32)
        bias_ref[:, pl.ds(v_column, 128)] = jnp.broadcast_to(
            jnp.sum(d_value, axis=0, keepdims=True), (8, 128)
        )


def attention_backward(qkv, attended, d_attended, lse, segments, ranges, head_size):
    rows, width = qkv.shape
    groups = width // 384
    blocks = -(-rows // BQ)
    padded = padded_rows(rows)
    heads = 128 // head_size
    seg_column = jnp.concatenate(
        [segments, jnp.full((blocks * BQ - rows,), 7, jnp.int32)]
    ).reshape(-1, 1)
    return pl.pallas_call(
        functools.partial(attention_backward_kernel, rows, head_size),
        grid_spec=pltpu.PrefetchScalarGridSpec(
            num_scalar_prefetch=1,
            grid=(groups, blocks),
            in_specs=[
                pl.BlockSpec((BQ, 128), lambda g, i, r: (i, g)),
                pl.BlockSpec((rows, 128), lambda g, i, r: (0, groups + g)),
                pl.BlockSpec((rows, 128), lambda g, i, r: (0, 2 * groups + g)),
                pl.BlockSpec((BQ, 128), lambda g, i, r: (i, g)),
                pl.BlockSpec((BQ, 128), lambda g, i, r: (i, g)),
                pl.BlockSpec((BQ, 128), lambda g, i, r: (i, g)),
                pl.BlockSpec((blocks * BQ, 1), lambda g, i, r: (0, 0)),
            ],
            out_specs=[
                pl.BlockSpec((rows, width), lambda g, i, r: (0, 0)),
                pl.BlockSpec((8, width), lambda g, i, r: (0, 0)),
            ],
            scratch_shapes=[
                pltpu.VMEM((padded, 256), jnp.bfloat16),
                pltpu.VMEM((padded, 256), jnp.bfloat16),
                pltpu.VMEM((heads * BQ, 256), jnp.bfloat16),
                pltpu.VMEM((heads * BQ, 256), jnp.bfloat16),
                pltpu.VMEM((128, BQ), jnp.bfloat16),
                pltpu.VMEM((128, BQ), jnp.bfloat16),
                pltpu.VMEM((128, padded), jnp.float32),
                pltpu.VMEM((128, padded), jnp.float32),
                pltpu.VMEM((heads * BQ, 128), jnp.float32),
            ],
        ),
        out_shape=[
            jax.ShapeDtypeStruct((rows, width), jnp.bfloat16),
            jax.ShapeDtypeStruct((8, width), jnp.float32),
        ],
        name="attention_backward",
    )(ranges, qkv, qkv, qkv, attended, d_attended, lse, seg_column)


EPSILON = 1e-06


def layer_norm(values, gain, bias):
    centre = jnp.mean(values, axis=-1, keepdims=True)
    centred = values - centre
    spread = jnp.mean(centred * centred, axis=-1, keepdims=True)
    return centred * lax.rsqrt(spread + EPSILON) * gain + bias


def split_heads(values, head_count):
    return values.reshape(
        values.shape[0], values.shape[1], head_count, values.shape[2] // head_count
    )


def forward_attention(queries, key_rows, value_rows, segments, head_count):
    strips_here, rows_here, model_width = queries.shape
    head_size = model_width // head_count
    scale = float(head_size) ** (-0.5)
    all_keys, all_values, all_segments = (
        lax.all_gather(key_rows, "blk", axis=1, tiled=True),
        lax.all_gather(value_rows, "blk", axis=1, tiled=True),
        lax.all_gather(segments, "blk", axis=1, tiled=True),
    )
    scores = (
        jnp.einsum(
            "srhd,skhd->srhk",
            split_heads(queries, head_count),
            split_heads(all_keys, head_count),
            preferred_element_type=jnp.float32,
        )
        * scale
    )
    allowed = segments[:, :, None, None] == all_segments[:, None, None, :]
    scores = jnp.where(allowed, scores, -1e30)
    peak = jnp.max(scores, axis=-1)
    raised = jnp.where(allowed, jnp.exp(scores - peak[..., None]), 0.0)
    total = jnp.sum(raised, axis=-1)
    probs = (raised / total[..., None]).astype(jnp.bfloat16)
    weighted = jnp.einsum(
        "srhk,skhd->srhd",
        probs,
        split_heads(all_values, head_count),
        preferred_element_type=jnp.float32,
    )
    attended = weighted.reshape(strips_here, rows_here, model_width)
    logsum = peak + jnp.log(total)
    return (attended, logsum, (all_keys, all_values, all_segments))


def gradient_terms(
    queries,
    out_grad,
    logsum,
    row_dots,
    query_segments,
    key_rows,
    value_rows,
    key_segments,
    head_count,
):
    strips_here, rows_here, model_width = queries.shape
    key_count = key_rows.shape[1]
    query_heads = split_heads(queries, head_count)
    grad_heads = split_heads(out_grad, head_count)
    key_heads = split_heads(key_rows, head_count)
    value_heads = split_heads(value_rows, head_count)
    scale = float(query_heads.shape[-1]) ** (-0.5)
    scores = (
        jnp.einsum("srhd,skhd->srhk", query_heads, key_heads, preferred_element_type=jnp.float32)
        * scale
    )
    allowed = query_segments[:, :, None, None] == key_segments[:, None, None, :]
    probs = jnp.where(allowed, jnp.exp(scores - logsum[..., None]), 0.0)
    prob_grads = jnp.einsum(
        "srhd,skhd->srhk", grad_heads, value_heads, preferred_element_type=jnp.float32
    )
    score_grads = (probs * (prob_grads - row_dots[..., None])).astype(jnp.bfloat16)
    d_query = (
        jnp.einsum("srhk,skhd->srhd", score_grads, key_heads, preferred_element_type=jnp.float32)
        * scale
    )
    d_key = (
        jnp.einsum("srhk,srhd->skhd", score_grads, query_heads, preferred_element_type=jnp.float32)
        * scale
    )
    d_value = jnp.einsum(
        "srhk,srhd->skhd",
        probs.astype(jnp.bfloat16),
        grad_heads,
        preferred_element_type=jnp.float32,
    )
    return (
        d_query.reshape(strips_here, rows_here, model_width),
        d_key.reshape(strips_here, key_count, model_width),
        d_value.reshape(strips_here, key_count, model_width),
    )


def backward_attention(queries, segments, gathered, out_grad, attended, logsum, head_count):
    row_dots = jnp.sum(
        split_heads(out_grad.astype(jnp.float32), head_count) * split_heads(attended, head_count),
        axis=-1,
    )
    all_keys, all_values, all_segments = gathered
    d_query, key_terms, value_terms = gradient_terms(
        queries,
        out_grad,
        logsum,
        row_dots,
        segments,
        all_keys,
        all_values,
        all_segments,
        head_count,
    )
    d_key, d_value = (
        lax.psum_scatter(
            key_terms.astype(jnp.bfloat16), "blk", scatter_dimension=1, tiled=True
        ).astype(jnp.float32),
        lax.psum_scatter(
            value_terms.astype(jnp.bfloat16), "blk", scatter_dimension=1, tiled=True
        ).astype(jnp.float32),
    )
    return (d_query, d_key, d_value)


def block_forward(residual, segments, weights, head_count):
    (
        norm1_gain,
        norm1_bias,
        qkv_weight,
        query_bias,
        value_bias,
        out_weight,
        out_bias,
        norm2_gain,
        norm2_bias,
        up_weight,
        up_bias,
        down_weight,
        down_bias,
    ) = weights
    model_width = residual.shape[-1]
    normed = layer_norm(
        residual, norm1_gain.astype(jnp.float32), norm1_bias.astype(jnp.float32)
    ).astype(jnp.bfloat16)
    projected = jnp.dot(normed, qkv_weight, preferred_element_type=jnp.float32)
    queries = (projected[..., :model_width] + query_bias.astype(jnp.float32)).astype(jnp.bfloat16)
    key_rows = projected[..., model_width : 2 * model_width].astype(jnp.bfloat16)
    value_rows = (projected[..., 2 * model_width :] + value_bias.astype(jnp.float32)).astype(
        jnp.bfloat16
    )
    attended, logsum, gathered = forward_attention(
        queries, key_rows, value_rows, segments, head_count
    )
    attended_low = attended.astype(jnp.bfloat16)
    middle = residual + (
        jnp.dot(attended_low, out_weight, preferred_element_type=jnp.float32)
        + out_bias.astype(jnp.float32)
    )
    normed_two = layer_norm(
        middle, norm2_gain.astype(jnp.float32), norm2_bias.astype(jnp.float32)
    ).astype(jnp.bfloat16)
    pre_act = jnp.dot(normed_two, up_weight, preferred_element_type=jnp.float32) + up_bias.astype(
        jnp.float32
    )
    hidden = jax.nn.gelu(pre_act, approximate=False).astype(jnp.bfloat16)
    result = middle + (
        jnp.dot(hidden, down_weight, preferred_element_type=jnp.float32)
        + down_bias.astype(jnp.float32)
    )
    kept = (
        residual,
        normed,
        queries,
        key_rows,
        value_rows,
        gathered,
        attended,
        logsum,
        attended_low,
        middle,
        normed_two,
        pre_act,
        hidden,
    )
    return (result, kept)


def block_backward(upstream, kept, weights, segments, head_count):
    (
        norm1_gain,
        norm1_bias,
        qkv_weight,
        query_bias,
        value_bias,
        out_weight,
        out_bias,
        norm2_gain,
        norm2_bias,
        up_weight,
        up_bias,
        down_weight,
        down_bias,
    ) = weights
    (
        residual,
        normed,
        queries,
        key_rows,
        value_rows,
        gathered,
        attended,
        logsum,
        attended_low,
        middle,
        normed_two,
        pre_act,
        hidden,
    ) = kept
    d_down = upstream.astype(jnp.bfloat16)
    grad_down_bias = jnp.sum(d_down.astype(jnp.float32), axis=(0, 1))
    grad_down = jnp.einsum("srf,srw->fw", hidden, d_down, preferred_element_type=jnp.float32)
    d_hidden = jnp.einsum("srw,fw->srf", d_down, down_weight, preferred_element_type=jnp.float32)
    unused_act, gelu_pull = jax.vjp(
        lambda inner_vals: jax.nn.gelu(inner_vals, approximate=False), pre_act
    )
    d_pre = gelu_pull(d_hidden)[0].astype(jnp.bfloat16)
    grad_up_bias = jnp.sum(d_pre.astype(jnp.float32), axis=(0, 1))
    grad_up = jnp.einsum("srw,srf->wf", normed_two, d_pre, preferred_element_type=jnp.float32)
    d_normed_two = jnp.einsum("srf,wf->srw", d_pre, up_weight, preferred_element_type=jnp.float32)
    unused_two, norm_two_pull = jax.vjp(
        layer_norm, middle, norm2_gain.astype(jnp.float32), norm2_bias.astype(jnp.float32)
    )
    d_middle, grad_norm2_gain, grad_norm2_bias = norm_two_pull(d_normed_two)
    d_middle = d_middle + upstream
    d_branch = d_middle.astype(jnp.bfloat16)
    grad_out_bias = jnp.sum(d_branch.astype(jnp.float32), axis=(0, 1))
    grad_out = jnp.einsum("srw,srv->wv", attended_low, d_branch, preferred_element_type=jnp.float32)
    d_attended = jnp.einsum(
        "srv,wv->srw", d_branch, out_weight, preferred_element_type=jnp.float32
    ).astype(jnp.bfloat16)
    d_query, d_key, d_value = backward_attention(
        queries, segments, gathered, d_attended, attended, logsum, head_count
    )
    d_query = d_query.astype(jnp.bfloat16)
    d_key = d_key.astype(jnp.bfloat16)
    d_value = d_value.astype(jnp.bfloat16)
    grad_query_bias = jnp.sum(d_query.astype(jnp.float32), axis=(0, 1))
    grad_value_bias = jnp.sum(d_value.astype(jnp.float32), axis=(0, 1))
    d_projected = jnp.concatenate([d_query, d_key, d_value], axis=-1)
    grad_qkv = jnp.einsum("srw,srx->wx", normed, d_projected, preferred_element_type=jnp.float32)
    d_normed = jnp.einsum(
        "srx,wx->srw", d_projected, qkv_weight, preferred_element_type=jnp.float32
    )
    unused_one, norm_one_pull = jax.vjp(
        layer_norm, residual, norm1_gain.astype(jnp.float32), norm1_bias.astype(jnp.float32)
    )
    d_residual, grad_norm1_gain, grad_norm1_bias = norm_one_pull(d_normed)
    d_residual = d_residual + d_middle
    gradients = (
        grad_norm1_gain,
        grad_norm1_bias,
        grad_qkv,
        grad_query_bias,
        grad_value_bias,
        grad_out,
        grad_out_bias,
        grad_norm2_gain,
        grad_norm2_bias,
        grad_up,
        grad_up_bias,
        grad_down,
        grad_down_bias,
    )
    return (d_residual, gradients)


def reduce_gradients(gradients):
    dp_count = lax.axis_size("dp")
    blk_count = lax.axis_size("blk")
    packed = jnp.concatenate([gradient.reshape(dp_count, -1) for gradient in gradients], axis=1)
    width_all = packed.shape[1]
    stacked = packed.reshape(dp_count * blk_count, width_all // blk_count)
    share = lax.psum_scatter(stacked, ("dp", "blk"), scatter_dimension=0, tiled=True)
    summed = (
        lax.all_gather(share.astype(jnp.bfloat16), "blk", axis=0, tiled=True)
        .astype(share.dtype)
        .reshape(1, width_all)
    )
    flattened = summed.reshape(-1)
    shares = []
    offset = 0
    for gradient in gradients:
        length = gradient.size // dp_count
        shape_here = (gradient.shape[0] // dp_count,) + gradient.shape[1:]
        shares.append(flattened[offset : offset + length].reshape(shape_here))
        offset = offset + length
    return tuple(shares)


def per_device(
    patches,
    vis_slot,
    seg_ids,
    enc_norm1_gain,
    enc_norm1_bias,
    enc_qkv_weight,
    enc_query_bias,
    enc_value_bias,
    enc_out_weight,
    enc_out_bias,
    enc_norm2_gain,
    enc_norm2_bias,
    enc_up_weight,
    enc_up_bias,
    enc_down_weight,
    enc_down_bias,
    emb_weight,
    emb_bias,
    mask_token,
    dec_norm1_gain,
    dec_norm1_bias,
    dec_qkv_weight,
    dec_query_bias,
    dec_value_bias,
    dec_out_weight,
    dec_out_bias,
    dec_norm2_gain,
    dec_norm2_bias,
    dec_up_weight,
    dec_up_bias,
    dec_down_weight,
    dec_down_bias,
    cotangent,
):
    enc_weights = (
        enc_norm1_gain,
        enc_norm1_bias,
        enc_qkv_weight,
        enc_query_bias,
        enc_value_bias,
        enc_out_weight,
        enc_out_bias,
        enc_norm2_gain,
        enc_norm2_bias,
        enc_up_weight,
        enc_up_bias,
        enc_down_weight,
        enc_down_bias,
    )
    dec_weights = (
        dec_norm1_gain,
        dec_norm1_bias,
        dec_qkv_weight,
        dec_query_bias,
        dec_value_bias,
        dec_out_weight,
        dec_out_bias,
        dec_norm2_gain,
        dec_norm2_bias,
        dec_up_weight,
        dec_up_bias,
        dec_down_weight,
        dec_down_bias,
    )
    vis_segments = jnp.take_along_axis(seg_ids, vis_slot, axis=1)
    encoded, enc_kept = block_forward(
        patches.astype(jnp.float32), vis_segments, enc_weights, HEADS_ENC
    )
    encoded_low = encoded.astype(jnp.bfloat16)
    span_rows = seg_ids.shape[1]
    onehot = (vis_slot[:, None, :] == lax.broadcasted_iota(jnp.int32, (1, span_rows, 1), 1)).astype(
        jnp.bfloat16
    )
    placed = jnp.einsum(
        "spv,sve->spe", onehot, encoded_low, preferred_element_type=jnp.float32
    ).astype(jnp.bfloat16)
    visible_rows = jnp.sum(onehot.astype(jnp.float32), axis=-1)[..., None]
    dec_in = (
        jnp.dot(placed, emb_weight, preferred_element_type=jnp.float32)
        + visible_rows * emb_bias.astype(jnp.float32)
        + (1.0 - visible_rows) * mask_token.astype(jnp.float32)
    )
    decoded, dec_kept = block_forward(dec_in, seg_ids, dec_weights, HEADS_DEC)
    d_dec_in, dec_grads = block_backward(
        cotangent.astype(jnp.float32), dec_kept, dec_weights, seg_ids, HEADS_DEC
    )
    grad_emb_bias = jnp.sum(d_dec_in * visible_rows, axis=(0, 1))
    grad_mask = jnp.sum(d_dec_in * (1.0 - visible_rows), axis=(0, 1))
    d_dec_low = d_dec_in.astype(jnp.bfloat16)
    grad_emb = jnp.einsum("spe,spc->ec", placed, d_dec_low, preferred_element_type=jnp.float32)
    d_placed = jnp.einsum("spc,ec->spe", d_dec_low, emb_weight, preferred_element_type=jnp.float32)
    d_encoded = jnp.take_along_axis(d_placed, vis_slot[..., None], axis=1)
    d_patches, enc_grads = block_backward(d_encoded, enc_kept, enc_weights, vis_segments, HEADS_ENC)
    gradients = enc_grads + (grad_emb, grad_emb_bias, grad_mask) + dec_grads
    shares = reduce_gradients(gradients)
    return (decoded.astype(jnp.bfloat16), d_patches.astype(jnp.bfloat16)) + shares


def pairs(count):
    return [(i, i ^ 1) for i in range(count)]


def to_partner(values):
    return lax.ppermute(values, "dp", pairs(lax.axis_size("dp")))


def relocate(values):
    moves = []
    for d in range(lax.axis_size("dp")):
        for y in range(2):
            moves.append((d * 2 + y, ((d & ~1) | y) * 2 + (d & 1)))
    return lax.ppermute(values, ("dp", "blk"), moves)


def join(mine, other, core, axis):
    return jnp.where(
        core == 0,
        jnp.concatenate([mine, other], axis=axis),
        jnp.concatenate([other, mine], axis=axis),
    )


def half(values, which, axis):
    size = values.shape[axis] // 2
    return lax.dynamic_slice_in_dim(values, which * size, size, axis)


def own_heads(weight, core, parts):
    width = weight.shape[-1] // (2 * parts)
    split = weight.reshape(weight.shape[:-1] + (parts, 2, width))
    picked = lax.dynamic_index_in_dim(split, core, axis=split.ndim - 2, keepdims=False)
    return picked.reshape(weight.shape[:-1] + (parts * width,))


def norm_parts(values):
    centred = values - jnp.mean(values, axis=-1, keepdims=True)
    spread = jnp.mean(centred * centred, axis=-1, keepdims=True)
    return centred * lax.rsqrt(spread + EPSILON), lax.rsqrt(spread + EPSILON)


def norm_backward(values, gain, upstream):
    normal, inverse = norm_parts(values)
    weighted = upstream * gain
    lean = jnp.mean(weighted, axis=-1, keepdims=True)
    along = jnp.mean(weighted * normal, axis=-1, keepdims=True)
    return (
        inverse * (weighted - lean - normal * along),
        jnp.sum(upstream * normal, axis=0),
        jnp.sum(upstream, axis=0),
    )


def wide(values):
    return values.astype(jnp.float32)


def low(values):
    return values.astype(jnp.bfloat16)


def times(left, right):
    return jnp.dot(left, right, preferred_element_type=jnp.float32)


def times_t(left, right):
    return lax.dot_general(left, right, NT, preferred_element_type=jnp.float32)


def t_times(left, right):
    return lax.dot_general(left, right, (((0,), (0,)), ((), ())), preferred_element_type=jnp.float32)


def strip_forward(residual, segments, ranges, weights, head_count, core):
    (g1, b1, qkv_weight, q_bias, v_bias, out_w, out_b, g2, b2, up_w, up_b, down_w, down_b) = weights
    width = residual.shape[-1]
    head_size = width // head_count
    own = width // 2
    normed = low(layer_norm(residual, wide(g1), wide(b1)))
    qkv_own = own_heads(qkv_weight, core, 3)
    bias_own = jnp.concatenate(
        [half(wide(q_bias), core, 0), jnp.zeros((own,), jnp.float32), half(wide(v_bias), core, 0)]
    )
    factor = jnp.where(jnp.arange(3 * own) < own, float(head_size) ** -0.5 / LN2, 1.0)
    normed_all = join(normed, to_partner(normed), core, 0)
    qkv = low((times(normed_all, qkv_own) + bias_own) * factor)
    attended_own, logsum = attention_forward(qkv, segments, ranges, head_size)
    received = to_partner(half(attended_own, 1 - core, 0))
    attended = join(half(attended_own, core, 0), received, core, 1)
    middle = residual + (times(attended, out_w) + wide(out_b))
    normed_two = low(layer_norm(middle, wide(g2), wide(b2)))
    pre_act = times(normed_two, up_w) + wide(up_b)
    hidden = low(jax.nn.gelu(pre_act, approximate=False))
    result = middle + (times(hidden, down_w) + wide(down_b))
    kept = (
        residual, normed_all, qkv_own, qkv, attended_own, logsum, attended, middle,
        normed_two, pre_act, hidden,
    )
    return result, kept


def strip_backward(upstream, kept, weights, segments, ranges, head_count, core):
    (g1, b1, qkv_weight, q_bias, v_bias, out_w, out_b, g2, b2, up_w, up_b, down_w, down_b) = weights
    (
        residual, normed_all, qkv_own, qkv, attended_own, logsum, attended, middle,
        normed_two, pre_act, hidden,
    ) = kept
    width = residual.shape[-1]
    own = width // 2
    d_down = low(upstream)
    grad_down_b = jnp.sum(wide(d_down), axis=0)
    grad_down = share_of(low(t_times(hidden, d_down)), core)
    d_hidden = times_t(d_down, down_w)
    _, pull = jax.vjp(lambda u: jax.nn.gelu(u, approximate=False), pre_act)
    d_pre = low(pull(d_hidden)[0])
    grad_up_b = jnp.sum(wide(d_pre), axis=0)
    grad_up = share_of(low(t_times(normed_two, d_pre)), core)
    d_normed_two = times_t(d_pre, up_w)
    d_middle, grad_g2, grad_b2 = norm_backward(middle, wide(g2), d_normed_two)
    d_middle = d_middle + upstream
    d_branch = low(d_middle)
    grad_out_b = jnp.sum(wide(d_branch), axis=0)
    grad_out = share_of(low(t_times(attended, d_branch)), core)
    d_attended = low(times_t(d_branch, out_w))
    received = to_partner(half(d_attended, 1 - core, 1))
    d_attended_own = join(half(d_attended, core, 1), received, core, 0)
    d_qkv, bias_sums = attention_backward(
        qkv, attended_own, d_attended_own, logsum, segments, ranges, width // head_count
    )
    bias_sums = bias_sums[0]
    nothing = jnp.zeros((own,), jnp.float32)
    grad_q_b = join(bias_sums[:own], nothing, core, 0)
    grad_v_b = join(bias_sums[2 * own :], nothing, core, 0)
    partial = times_t(d_qkv, qkv_own)
    other = to_partner(low(half(partial, 1 - core, 0)))
    d_normed = half(partial, core, 0) + wide(other)
    grad_qkv = head_share_of(low(t_times(normed_all, d_qkv)), core)
    d_residual, grad_g1, grad_b1 = norm_backward(residual, wide(g1), d_normed)
    small = (grad_g1, grad_b1, grad_q_b, grad_v_b, grad_out_b, grad_g2, grad_b2, grad_up_b, grad_down_b)
    return d_residual + d_middle, (grad_qkv, grad_out, grad_up, grad_down), small


def core_rows(grad, core):
    count = lax.axis_size("dp") // 2
    rows = grad.shape[0] // (2 * count)
    split = grad.reshape(count, 2, rows, grad.shape[1])
    keep = lax.dynamic_index_in_dim(split, core, axis=1, keepdims=False)
    send = lax.dynamic_index_in_dim(split, 1 - core, axis=1, keepdims=False)
    return keep, to_partner(send)


def reduce_chips(total):
    size = lax.axis_size("dp")
    groups = [list(range(0, size, 2)), list(range(1, size, 2))]
    share = lax.psum_scatter(
        total.reshape(-1, total.shape[-1]), "dp", scatter_dimension=0,
        axis_index_groups=groups, tiled=True,
    )
    return wide(share) + wide(lax.ppermute(share, "blk", [(0, 1), (1, 0)]))


def share_of(grad, core):
    keep, got = core_rows(grad, core)
    return reduce_chips(low(wide(keep) + wide(got)))


def head_share_of(grad, core):
    keep, got = core_rows(grad, core)
    shape = keep.shape[:2] + (3, 1, keep.shape[2] // 3)
    total = join(keep.reshape(shape), got.reshape(shape), core, 3)
    return reduce_chips(total.reshape(keep.shape[:2] + (-1,)))


def small_shares(small):
    size = lax.axis_size("dp")
    packed = jnp.concatenate([grad.reshape(size, -1) for grad in small], axis=1)
    total = lax.psum(packed, ("dp", "blk"))
    mine = lax.dynamic_index_in_dim(total, lax.axis_index("dp"), axis=0, keepdims=False)
    shares, at = [], 0
    for grad in small:
        length = grad.shape[0] // size
        shares.append(mine[at : at + length])
        at = at + length
    return shares


def ordered(large, small):
    qkv, out, up, down = large
    g1, b1, q_b, v_b, out_b, g2, b2, up_b, down_b = small
    return (g1, b1, qkv, q_b, v_b, out, out_b, g2, b2, up, up_b, down, down_b)


def chip_device(patches, vis_slot, seg_ids, *rest):
    enc_weights, (emb_weight, emb_bias, mask_token) = rest[0:13], rest[13:16]
    dec_weights, cotangent = rest[16:29], rest[29]
    core = lax.axis_index("dp") % 2
    span, visible = seg_ids.shape[1], vis_slot.shape[1]
    marks = relocate(jnp.concatenate([seg_ids[0], vis_slot[0]]))
    rows = relocate(patches[0])
    seg_here, slots = marks[:span], marks[span:]
    chosen = slots[None, :] == lax.broadcasted_iota(jnp.int32, (span, visible), 0)
    vis_here = jnp.sum(jnp.where(chosen, seg_here[:, None], 0), axis=0)
    both = jnp.concatenate([seg_here, vis_here])
    across = to_partner(both)
    segments = join(both[:span], across[:span], core, 0)
    vis_segments = join(both[span:], across[span:], core, 0)
    ranges = key_ranges(segments, 2 * span)
    vis_ranges = key_ranges(vis_segments, 2 * visible)

    residual = wide(rows)
    encoded, enc_kept = strip_forward(
        residual, vis_segments, vis_ranges, enc_weights, HEADS_ENC, core
    )
    upstream, encoded = lax.optimization_barrier((cotangent[0], encoded))
    upstream = relocate(upstream)
    encoded_low = low(encoded)
    onehot = chosen.astype(jnp.bfloat16)
    placed = low(times(onehot, encoded_low))
    shown = jnp.sum(onehot.astype(jnp.float32), axis=1, keepdims=True)
    dec_in = (
        times(placed, emb_weight) + shown * wide(emb_bias) + (1.0 - shown) * wide(mask_token)
    )
    decoded, dec_kept = strip_forward(dec_in, segments, ranges, dec_weights, HEADS_DEC, core)
    dec_out = relocate(low(decoded))
    d_dec_in, dec_large, dec_small = strip_backward(
        wide(upstream), dec_kept, dec_weights, segments, ranges, HEADS_DEC, core
    )
    grad_emb_bias = jnp.sum(d_dec_in * shown, axis=0)
    grad_mask = jnp.sum(d_dec_in * (1.0 - shown), axis=0)
    d_shown = low(t_times(onehot, low(d_dec_in)))
    grad_emb = share_of(low(t_times(encoded_low, d_shown)), core)
    d_encoded = times_t(d_shown, emb_weight)
    d_rows, enc_large, enc_small = strip_backward(
        d_encoded, enc_kept, enc_weights, vis_segments, vis_ranges, HEADS_ENC, core
    )
    grad_patches = relocate(low(d_rows))
    dec_shares = small_shares(dec_small + (grad_emb_bias, grad_mask))
    enc_shares = small_shares(enc_small)
    return (
        (dec_out[None], grad_patches[None])
        + ordered(enc_large, enc_shares)
        + (grad_emb, dec_shares[9], dec_shares[10])
        + ordered(dec_large, dec_shares[:9])
    )


def solution(mesh):
    one_strip_a_core = mesh.shape["blk"] == 2
    return jax.shard_map(
        chip_device if one_strip_a_core else per_device,
        mesh=mesh,
        in_specs=(
            P("dp", "blk", None),
            P("dp", "blk"),
            P("dp", "blk"),
            P(),
            P(),
            P(),
            P(),
            P(),
            P(),
            P(),
            P(),
            P(),
            P(),
            P(),
            P(),
            P(),
            P(),
            P(),
            P(),
            P(),
            P(),
            P(),
            P(),
            P(),
            P(),
            P(),
            P(),
            P(),
            P(),
            P(),
            P(),
            P(),
            P("dp", "blk", None),
        ),
        out_specs=(
            P("dp", "blk", None),
            P("dp", "blk", None),
            P("dp"),
            P("dp"),
            P("dp", None),
            P("dp"),
            P("dp"),
            P("dp", None),
            P("dp"),
            P("dp"),
            P("dp"),
            P("dp", None),
            P("dp"),
            P("dp", None),
            P("dp"),
            P("dp", None),
            P("dp"),
            P("dp"),
            P("dp"),
            P("dp"),
            P("dp", None),
            P("dp"),
            P("dp"),
            P("dp", None),
            P("dp"),
            P("dp"),
            P("dp"),
            P("dp", None),
            P("dp"),
            P("dp", None),
            P("dp"),
        ),
        check_vma=False,
    )
```
